32 devices in a mesh: dp: 4 (over x, core), ep: 8 (over z, y).
Axes of the slice: x: 2, y: 2, z: 4, core: 2. Of those that a mesh axis runs over, the one named last changes fastest.
Arguments:
- tokens: bfloat16 [4096, 2048], P(('dp', 'ep')), parts along dimension 0, may hold values from -6 to 6
- expert_ids: int32 [4096, 8], P(('dp', 'ep')), parts along dimension 0, may hold values from 0 to 15, all different within a row; in each aligned block of 32 rows (0 to 31, 32 to 63, ...) at most 32 rows name the same one
- gate_nums: int32 [4096, 8], P(('dp', 'ep')), parts along dimension 0, may hold values from 64 to 1023
- w_gate: bfloat16 [16, 2048, 768], P('ep'), may hold values from -0.125 to 0.125
- w_up: bfloat16 [16, 2048, 768], P('ep'), may hold values from -0.125 to 0.125
- w_down: bfloat16 [16, 768, 2048], P('ep'), may hold values from -0.21875 to 0.21875
Outputs:
- mixed: bfloat16 [4096, 2048], P(('dp', 'ep')), parts along dimension 0
The draws below stay inside these ranges and needn't reach their ends.
There are 4 independent parts, one for each index of `dp`. The reference program is written for one: setup_inputs(seed, part) draws one part's arguments, and reference() takes and returns one part's arrays. A program takes and returns all parts, laid end to end along the dimension named above; an argument that names none is the same for every part. Nothing has to cross between parts.
Inputs may be any that keep to these rules, and one draw needn't show every extreme that they name: `expert_ids`: each row names 8 different experts. In every aligned block of 32 rows no expert is named by more than 32 rows, a bound that some block reaches.
All inputs are finite; a program needn't handle non-finite values.
Results may differ from the reference program's by a relative error of at most 0.008.
Values may be sent and summed in bfloat16 or wider, within the bound.
A program may use at most 128 MiB of HBM per device.

```python
import math
import jax
import jax.numpy as jnp
import numpy as np
from jax import lax

D = 2048
FF = 768
TOP = 8
EXPERTS = 16
TOKENS = 1024
BLK = 32
CAP = 32


def touch_ends(array, own_key, least, high):
    extent = array.shape
    place = [jax.random.randint(jax.random.fold_in(own_key, axis), (), 0, extent[axis]) for axis in range(len(extent))]
    array = array.at[tuple(place)].set(least)
    longest = extent.index(max(extent))
    place[longest] = (place[longest] + 1) % extent[longest]
    return array.at[tuple(place)].set(high)


def steps_of(own_key, shape, split, low, largest):
    def one(axis_at, parts):
        steps = jax.random.uniform(jax.random.fold_in(jax.random.fold_in(own_key, 6), axis_at), (parts,), jnp.float32, low / len(split), largest / len(split))
        return jnp.repeat(jnp.exp(steps), shape[axis_at] // parts).reshape((-1,) + (1,) * (len(shape) - axis_at - 1))

    level = one(*split[0])
    for cut in split[1:]:
        level = level * one(*cut)
    return level


def deal_out(own_key, own, number, rows, count, top, most, lean):
    order = jax.random.permutation(own_key, count)
    heavy_load, ordinary = shares(count, rows * top, most, lean, True), shares(count, rows * top, most, lean, False)
    places = jnp.arange(count)

    def named(tallies, rotation):
        used = int((tallies > 0).sum())
        fixed = max(1, used // 4)
        moved = fixed + (places - fixed + rotation * (used - fixed)) % max(1, count - fixed)
        return jnp.zeros((count,), jnp.int32).at[order[jnp.where(places < fixed, places, moved)]].set(jnp.asarray(tallies, jnp.int32))

    tallies = jnp.where(number % 4 == 0, named(heavy_load, number // 4), named(ordinary, number - number // 4 - 1))
    mixed = jax.random.permutation(jax.random.fold_in(own, 3), count)
    source_of, sink = mixed[0:count // 2 * 2:2], mixed[1:count // 2 * 2:2]
    margin = jnp.minimum(tallies[source_of] - 1, most - tallies[sink]) // 2
    margin = jnp.where((source_of == order[0]) | (sink == order[0]) | (tallies[sink] == 0), 0, jnp.maximum(margin, 0))
    moved = jax.random.randint(jax.random.fold_in(own, 4), (count // 2,), 0, 1 << 20) % (margin + 1)
    tallies = tallies.at[source_of].add(-moved).at[sink].add(moved)
    members = jnp.searchsorted(jnp.cumsum(tallies), jnp.arange(rows * top), side="right").astype(jnp.int32)
    table = members.reshape(top, rows).T
    table = table[jax.random.permutation(jax.random.fold_in(own, 1), rows)]
    rotation = jax.random.randint(jax.random.fold_in(own, 2), (rows, 1), 0, top)
    return jnp.take_along_axis(table, (jnp.arange(top)[None, :] + rotation) % top, axis=1)


def shares(amount, total, bound, lean, full):
    loads = [(1 << 20) // math.isqrt(rank ** lean) + 1 for rank in range(1, amount + 1)]
    largest = bound if full else min(bound, max(-(-total // amount), total * loads[0] // sum(loads)))
    least = 1 if total - largest >= amount - 1 else 0
    holding, surplus = [largest] + [least] * (amount - 1), total - largest - least * (amount - 1)
    while surplus > 0:
        movable = [i for i in range(1, amount) if holding[i] < largest] or [i for i in range(1, amount) if holding[i] < bound]
        mass, budget = sum([loads[i] for i in movable]), surplus
        for i in movable:
            addition = min(bound - holding[i], max(1, budget * loads[i] // mass), surplus)
            holding[i] = holding[i] + addition
            surplus = surplus - addition
    return np.array(holding)


def noise(rng, extent, deviation, limit, shards=(), held_as=jnp.bfloat16):
    entries = deviation * jax.random.normal(rng, extent, jnp.float32)
    if shards:
        entries = entries * steps_of(rng, extent, shards, -0.22, 0.18)
    return jnp.clip(entries, -limit, limit).astype(held_as)


def setup_inputs(seed: int = 0, part: int = 0) -> dict:
    keys = jax.random.split(jax.random.key(seed), 7)
    part_keys = jax.random.split(jax.random.fold_in(keys[6], part), 7)
    tokens = noise(part_keys[0], (TOKENS, D), 1.0, 6.0, ((0, 8),))
    expert_ids_keys = jax.random.split(jax.random.fold_in(part_keys[1], 1), TOKENS // BLK)
    expert_ids_turns = jax.random.permutation(jax.random.fold_in(part_keys[1], 3), TOKENS // BLK)
    expert_ids = jax.vmap(lambda own, number: deal_out(jax.random.fold_in(part_keys[1], 2), own, number, BLK, EXPERTS, TOP, CAP, 2))(expert_ids_keys, expert_ids_turns).reshape((TOKENS, TOP))
    gate_nums = touch_ends(jax.random.randint(part_keys[2], (TOKENS, TOP), 64, 1024), jax.random.fold_in(part_keys[2], 1), 64, 1023).astype(jnp.int32)
    w_gate = noise(keys[3], (EXPERTS, D, FF), D ** -0.5, 0.125, ((0, 8),))
    w_up = noise(keys[4], (EXPERTS, D, FF), D ** -0.5, 0.125, ((0, 8),))
    w_down = noise(keys[5], (EXPERTS, FF, D), FF ** -0.5, 0.21875, ((0, 8),))
    return {"tokens": tokens, "expert_ids": expert_ids, "gate_nums": gate_nums, "w_gate": w_gate, "w_up": w_up, "w_down": w_down}


denominator = 1024.0


def reference(tokens, expert_ids, gate_nums, w_gate, w_up, w_down):
    total = tokens.shape[0]
    most = CAP * (total // BLK)
    gates = gate_nums.astype(jnp.float32) / denominator

    def step(accum, expert):
        hit = expert_ids == expert
        weight = jnp.sum(jnp.where(hit, gates, jnp.zeros_like(gates)), axis=1)
        member = jnp.any(hit, axis=1)
        index = jnp.nonzero(member, size=most, fill_value=0)[0].astype(jnp.int32)
        valid = jnp.arange(most, dtype=jnp.int32) < jnp.sum(member.astype(jnp.int32))
        picked = tokens[index]
        gate = jnp.dot(picked, w_gate[expert], preferred_element_type=jnp.float32)
        up = jnp.dot(picked, w_up[expert], preferred_element_type=jnp.float32)
        hidden = (jax.nn.silu(gate) * up).astype(jnp.bfloat16)
        result = jnp.dot(hidden, w_down[expert], preferred_element_type=jnp.float32).astype(jnp.bfloat16)
        scale = jnp.where(valid, weight[index], jnp.zeros_like(weight[index]))
        accum = accum.at[index].add(scale[:, None] * result.astype(jnp.float32))
        return accum, None

    start = jnp.zeros((total, tokens.shape[1]), jnp.float32)
    accum, _ = lax.scan(step, start, jnp.arange(EXPERTS, dtype=jnp.int32))
    return accum.astype(jnp.bfloat16)
```

```python
import functools

import jax
import jax.numpy as jnp
from jax import lax
from jax.experimental import pallas as pl
from jax.experimental.pallas import tpu as pltpu
from jax.sharding import PartitionSpec as P

denominator = 1024.0
SIDE = 2
LANES = 256
VMEM = 60 * 2**20

AWAY, HOME, ACROSS = 0, 1, 2
UNITS = 8
PIECES = 4
ROUNDS = (
    ((0, 0), (1, 0), (2, 0), (2, 1), (0, 1), (3, 0), (3, 1), (1, 1)),
    ((1, 0), (2, 1), (0, 1), (0, 0), (2, 0), (1, 1), (3, 0), (3, 1)),
)
SENDS = (
    (
        (10000, 10002, 10010, 10022, 10020, 10032, 10030, 11002, 10040, 11012, 10050, 11022, 10060, 10042,
         10070, 10052, 11100, 12002, 10130, 12012, 12022, 10150),
        (),
        (12100, 11032),
        (),
        (11042, 20100, 20110, 12032, 20120, 12042),
        (12052,),
        (),
        (),
        (21100, 21132, 21110),
        (),
        (21120, 12062),
        (),
        (22112, 22000, 22122, 21000, 22132, 12072, 22010, 13002, 22020, 13012, 21010, 22030, 13022, 21020),
        (),
        (13042,),
        (),
        (21030, 22040, 22152),
        (22172,),
        (22100,),
        (),
        (20142,),
        (20152,),
        (22050, 20162),
        (),
        (22070, 23130, 23102),
        (23030,),
        (23122,),
        (),
        (23160, 23170, 11062, 11072, 23000, 23142, 23020, 23060, 23112, 23152),
        (),
        (23040, 20132),
        (),
        (23010, 20172, 23070, 23050, 22162, 21142, 22140, 21152, 30000, 21162, 30020, 22060, 21172, 30030,
         21040, 30040, 21050, 30010, 21060, 30050, 21070, 30060, 30070),
    ),
    (
        (11000, 11001, 11012, 11010, 11011, 11022, 11020, 11021, 11032, 11030, 12001, 10002, 11120, 12011,
         10012, 11130, 12021, 10022, 12012, 10100, 12031, 11040, 10111, 10042, 11050, 11031, 11042, 11060,
         11041, 10062, 11070, 12041, 10072, 10000, 12042, 12051),
        (10010, 12052),
        (10161,),
        (11062,),
        (10150, 10171, 10020, 12061, 11072, 10030, 12071, 13012, 11160, 13151, 13001, 13022, 11170, 10040,
         13011, 13032, 13021, 21102, 10050, 21110),
        (13131, 10060, 13031, 21122),
        (13042,),
        (10070, 13041),
        (22152, 22172),
        (12150,),
        (13051,),
        (),
        (13062, 13061),
        (),
        (13072, 13071),
        (),
        (20110, 20102, 20122),
        (13161,),
        (20142, 11151),
        (13171, 20152),
        (11051, 22130, 22030),
        (),
        (11061,),
        (22112,),
        (11071, 22102),
        (22122,),
        (21141, 22050),
        (),
        (22070, 22000, 23102, 23111),
        (23122, 21161),
        (22010,),
        (23132, 20131),
        (22020, 23142, 20171, 23160, 31000, 23152, 22161, 31010, 23172, 23000, 31020, 23030, 23020, 20162,
         21132, 20001, 21152, 23040, 20021, 21172, 23010, 20031, 23060, 23050, 20041, 31030, 23070, 20011,
         22142, 20051, 22060, 20061, 22040, 20071, 31050, 31060, 31040, 31070),
    ),
)


def expert_weights(expert_ids, gate_nums, experts):
    gates = gate_nums.astype(jnp.float32) / denominator
    labels = jnp.arange(experts, dtype=jnp.int32)
    onehot = expert_ids[:, :, None] == labels[None, None, :]
    return jnp.sum(jnp.where(onehot, gates[:, :, None], 0.0), axis=1)


def digits(code):
    return code // 10000, code // 1000 % 10, code // 100 % 10, code // 10 % 10, code % 10


def script(depth):
    acts, came = [], [{} for _ in SENDS]
    for role, pieces in enumerate(SENDS):
        seen, mine = set(), []
        for index, piece in enumerate(pieces):
            found = []

            def need(o, r, u):
                if (o, r) != (role, 0) and (o, r, u) not in seen:
                    seen.add((o, r, u))
                    found.append((0, o, r, u, ACROSS))

            for code in piece:
                kind, o, r, u, way = digits(code)
                if kind == 1:
                    need(o, r, u)
                found.append((kind, o, r, u, way))
                if kind != 2:
                    continue
                there, key = role + (way == AWAY) - (way == HOME), (o, r, u)
                if way == ACROSS:
                    key = (o, 1 - r, u)
                if there == depth // 2:
                    there, key, way = role, (depth - 1 - o, r, u), HOME
                came[there].setdefault(key, []).append(way)
            if index % PIECES == 0 and index < len(ROUNDS[role]) * PIECES:
                o, h = ROUNDS[role][index // PIECES]
                for r in range(SIDE):
                    for u in range(h * UNITS // 2, (h + 1) * UNITS // 2):
                        need(o, r, u)
            mine.append(found)
        acts.append(mine)
    return acts, came


def kernel(
    n, local,
    ids, nums, tokens, w_gate, w_up, w_down, out,
    rows, weights, factors, columns, gate, up, down, hidden, part, line, side,
    load_sem, weight_send, weight_recv, token_send, token_recv, result_send, line_recv, side_recv,
):
    depth = n // SIDE
    me = lax.axis_index("ep")
    z, y = me // SIDE, me % SIDE
    flip = z // (depth // 2)
    place = z + flip * (depth - 1 - 2 * z)
    count, width = tokens.shape
    ff = w_gate.shape[2]
    size = count // UNITS
    half = count // 2
    spots = depth * SIDE * UNITS
    acts, came = script(depth)
    steps = len(ROUNDS[0])

    def owner_of(o):
        return o + flip * (depth - 1 - 2 * o)

    def row_of(r):
        return y if r == 0 else 1 - y

    def offset(o, r, u):
        return owner_of(o) * SIDE * count + u * size // half * count + row_of(r) * half + u * size % half

    def spot(o, r, u):
        return (owner_of(o) * SIDE + row_of(r)) * UNITS + u

    def cut(start, extent=size):
        return pl.ds(pl.multiple_of(start, size), extent)

    def heading(way):
        return flip if way == AWAY else 1 - flip

    def device(way):
        return z * SIDE + 1 - y if way == ACROSS else me + SIDE * (1 - 2 * heading(way))

    def remote(source, target, send, recv, there):
        return pltpu.make_async_remote_copy(
            src_ref=source, dst_ref=target, send_sem=send, recv_sem=recv,
            device_id={"ep": there}, device_id_type=pl.DeviceIdType.MESH,
        )

    def token_copy(o, r, u, way):
        ref = rows.at[cut(offset(o, r, u))]
        return remote(ref, ref, token_send.at[way], token_recv.at[spot(o, r, u)], device(way))

    def landing(o, r, u, way):
        if way == ACROSS:
            return side.at[cut(owner_of(o) * count + u * size)], side_recv.at[owner_of(o) * UNITS + u]
        start = heading(way) * (depth * SIDE * count) + offset(o, r, u)
        return line.at[cut(start)], line_recv.at[heading(way) * spots + spot(o, r, u)]

    def result_copy(o, r, u, way):
        target, recv = landing(o, r, u, way)
        return remote(part.at[cut(offset(o, r, u))], target, result_send.at[way], recv, device(way))

    own = []
    for h in range(2):
        start = z * SIDE * count + h * count + y * half
        own.append(
            pltpu.make_async_copy(tokens.at[pl.ds(h * half, half)], rows.at[cut(start, half)], load_sem.at[h])
        )
    loads = []
    for e in range(local):
        loads.append(pltpu.make_async_copy(w_gate.at[e], gate.at[e], load_sem.at[2 + 3 * e]))
        loads.append(pltpu.make_async_copy(w_up.at[e], up.at[e], load_sem.at[3 + 3 * e]))
    for e in range(local):
        loads.append(pltpu.make_async_copy(w_down.at[e], down.at[pl.ds(e * ff, ff)], load_sem.at[4 + 3 * e]))
    for load in own + loads:
        load.start()

    barrier = pltpu.get_barrier_semaphore()
    for k in range(1, n):
        pl.semaphore_signal(
            barrier, inc=1, device_id={"ep": (me + k) % n}, device_id_type=pl.DeviceIdType.MESH
        )

    gates = nums[...].astype(jnp.float32) / denominator
    lanes = lax.broadcasted_iota(jnp.int32, weights.shape[1:], 0)
    for d in range(n):
        block = jnp.zeros(weights.shape[1:], jnp.float32)
        for e in range(local):
            chosen = jnp.sum(jnp.where(ids[...] == d * local + e, gates, 0.0), axis=0, keepdims=True)
            block = jnp.where(lanes == e, chosen, block)
        weights[d] = block
    factors[me] = weights[me]

    pl.semaphore_wait(barrier, n - 1)
    for load in own:
        load.wait()

    def act(role, kind, o, r, u, way):
        if kind == 0:
            token_copy(o, r, u, way).wait_recv()
            return
        if kind == 1:
            token_copy(o, r, u, way).start()
            return
        if kind == 3:
            o, r = role, 0
        mine = part.at[cut(offset(o, r, u))]
        ways = came[role].get((o, r, u), [])
        if ways:
            total = mine[...].astype(jnp.float32)
            for source in ways:
                target, recv = landing(o, r, u, source)
                remote(target, target, result_send.at[source], recv, device(source)).wait_recv()
                total = total + target[...].astype(jnp.float32)
            if kind == 2:
                mine[...] = total.astype(part.dtype)
        if kind == 2:
            result_copy(o, r, u, way).start()
        else:
            out[pl.ds(u * size, size)] = total.astype(out.dtype)

    def talk(p, i):
        for role, pieces in enumerate(acts):
            for step in range(steps):
                piece = pieces[step * PIECES + p]

                def body(role=role, piece=piece):
                    for action in piece:
                        act(role, *action)

                if piece:
                    pl.when((place == role) & (i == step))(body)

    def pick(i, which):
        found = jnp.int32(0)
        for role, rounds in enumerate(ROUNDS):
            for step, entry in enumerate(rounds):
                if entry[which]:
                    found = found + jnp.where((place == role) & (i == step), entry[which], 0)
        return found

    def weight_copy(k):
        there = (me + k) % n
        return remote(weights.at[there], factors.at[me], weight_send.at[0], weight_recv.at[me], there)

    for k in range(1, n):
        weight_copy(k).start()

    def ready():
        for k in range(1, n):
            source = (me + k) % n
            there = factors.at[source]
            remote(there, there, weight_send.at[0], weight_recv.at[source], source).wait_recv()
        for d in range(n):
            turned = factors[d].T
            for h in range(2):
                start = d // SIDE * SIDE * count + h * count + d % SIDE * half
                columns[pl.ds(start, half)] = turned[h * half : (h + 1) * half]

    def project(e, base):
        column = columns[cut(base, count), e : e + 1]

        def tile(t, carry):
            at = pl.ds(pl.multiple_of(t * LANES, LANES), LANES)
            block = rows[cut(base, count)]
            g = jnp.dot(block, gate[e, :, at], preferred_element_type=jnp.float32)
            v = jnp.dot(block, up[e, :, at], preferred_element_type=jnp.float32)
            h = g / (1.0 + jnp.exp(-g)) * v * column
            hidden[:, pl.ds(pl.multiple_of(e * ff + t * LANES, LANES), LANES)] = h.astype(jnp.bfloat16)
            return carry

        lax.fori_loop(0, ff // LANES, tile, 0, unroll=True)

    def spread(low, high, base):
        def tile(t, carry):
            at = pl.ds(pl.multiple_of(t * LANES, LANES), LANES)
            result = jnp.dot(hidden[...], down[:, at], preferred_element_type=jnp.float32)
            part[cut(base, count), at] = result.astype(jnp.bfloat16)
            return carry

        lax.fori_loop(low, high, tile, 0, unroll=True)

    def step(i, carry):
        o, h = pick(i, 0), pick(i, 1)
        base = owner_of(o) * SIDE * count + h * count
        tiles = width // LANES
        for p in range(PIECES):
            talk(p, i)

            @pl.when(i == 0)
            def _():
                if p == 0:
                    ready()
                for load in loads[2 * p : 2 * p + 2] if p < local else loads[2 * local :] if p == local else []:
                    load.wait()

            if p < local:
                project(p, base)
            else:
                share = tiles // (PIECES - local)
                spread((p - local) * share, (p - local + 1) * share, base)
        return carry

    lax.fori_loop(0, steps, step, 0)

    def ending(role):
        for piece in acts[role][steps * PIECES :]:
            for action in piece:
                act(role, *action)
        for way in (AWAY, HOME, ACROSS):
            for kind, sems in ((1, token_send), (2, result_send)):
                sent = sum(a[0] == kind and a[4] == way for piece in acts[role] for a in piece)
                if sent:
                    all_of = rows.at[pl.ds(0, sent * size)]
                    remote(all_of, all_of, sems.at[way], token_recv.at[0], device(way)).wait_send()

    for role in range(len(acts)):
        pl.when(place == role)(functools.partial(ending, role))
    given = weights.at[pl.ds(0, n - 1)]
    remote(given, given, weight_send.at[0], weight_recv.at[0], device(ACROSS)).wait_send()


def fused(tokens, expert_ids, gate_nums, w_gate, w_up, w_down, n):
    count, width = tokens.shape
    local, _, ff = w_gate.shape
    depth = n // SIDE
    everyone = n * count
    kind = tokens.dtype
    dma = pltpu.SemaphoreType.DMA
    vmem = pl.BlockSpec(memory_space=pltpu.VMEM)
    hbm = pl.BlockSpec(memory_space=pl.ANY)
    return pl.pallas_call(
        functools.partial(kernel, n, local),
        out_shape=jax.ShapeDtypeStruct((count, width), kind),
        in_specs=[vmem, vmem, hbm, hbm, hbm, hbm],
        out_specs=vmem,
        scratch_shapes=[
            pltpu.VMEM((everyone, width), kind),
            pltpu.VMEM((n, 8, count), jnp.float32),
            pltpu.VMEM((n, 8, count), jnp.float32),
            pltpu.VMEM((everyone, 8), jnp.float32),
            pltpu.VMEM((local, width, ff), kind),
            pltpu.VMEM((local, width, ff), kind),
            pltpu.VMEM((local * ff, width), kind),
            pltpu.VMEM((count, local * ff), kind),
            pltpu.VMEM((everyone, width), kind),
            pltpu.VMEM((2 * everyone, width), kind),
            pltpu.VMEM((depth * count, width), kind),
            dma((2 + 3 * local,)),
            dma((1,)), dma((n,)),
            dma((3,)), dma((n * UNITS,)),
            dma((3,)), dma((2 * n * UNITS,)), dma((depth * UNITS,)),
        ],
        compiler_params=pltpu.CompilerParams(
            collective_id=0, has_side_effects=True, vmem_limit_bytes=VMEM
        ),
    )(expert_ids.T, gate_nums.T, tokens, w_gate, w_up, w_down)


def plain(tokens, expert_ids, gate_nums, w_gate, w_up, w_down, n):
    weight = expert_weights(expert_ids, gate_nums, w_gate.shape[0] * n)
    weights = lax.all_to_all(weight, "ep", split_axis=1, concat_axis=0, tiled=True)
    rows = lax.all_gather(tokens, "ep", axis=0, tiled=True)
    gate = jnp.einsum("td,xdf->xtf", rows, w_gate, preferred_element_type=jnp.float32)
    up = jnp.einsum("td,xdf->xtf", rows, w_up, preferred_element_type=jnp.float32)
    hidden = (jax.nn.silu(gate) * up * weights.T[:, :, None]).astype(jnp.bfloat16)
    result = jnp.einsum("xtf,xfd->td", hidden, w_down, preferred_element_type=jnp.float32)
    return lax.psum_scatter(
        result.astype(jnp.bfloat16), "ep", scatter_dimension=0, tiled=True
    )


def shards(n, tokens, expert_ids, gate_nums, w_gate, w_up, w_down):
    count, width = tokens.shape
    local, _, ff = w_gate.shape
    held = 5 * n * count * width + 3 * local * width * ff + 2 * count * local * ff
    fits = 2 * held < VMEM - 4 * 2**20
    planned = n == 2 * SIDE * len(SENDS) and PIECES == local + 2
    shaped = count % (16 * UNITS) == 0 and count % 128 == 0 and ff % LANES == 0 and width % (2 * LANES) == 0
    plan = fused if fits and planned and shaped else plain
    return plan(tokens, expert_ids, gate_nums, w_gate, w_up, w_down, n)


def solution(mesh):
    placed = (
        P(("dp", "ep"), None),
        P(("dp", "ep"), None),
        P(("dp", "ep"), None),
        P("ep", None, None),
        P("ep", None, None),
        P("ep", None, None),
    )
    return jax.shard_map(
        functools.partial(shards, mesh.shape["ep"]),
        mesh=mesh, in_specs=placed, out_specs=P(("dp", "ep"), None), check_vma=False,
    )
```

```python
import functools

import jax
import jax.numpy as jnp
from jax import lax
from jax.experimental import pallas as pl
from jax.experimental.pallas import tpu as pltpu
from jax.sharding import PartitionSpec as P

denominator = 1024.0
SIDE = 2
LANES = 256
VMEM = 60 * 2**20

AWAY, HOME, ACROSS = 0, 1, 2
UNITS = 8
PIECES = 4
ROUNDS = (
    ((1, 0), (2, 0), (0, 0), (0, 1), (3, 0), (3, 1), (2, 1), (1, 1)),
    ((0, 0), (1, 0), (3, 0), (2, 0), (3, 1), (2, 1), (0, 1), (1, 1)),
)
SENDS = (
    (
        (10003, 10002, 10032, 10023, 10045, 10100, 10043, 11005, 11025, 10143, 10063, 12005, 11100, 12025),
        (),
        (),
        (),
        (21122, 21103, 21130, 10065, 13002, 21003),
        (),
        (),
        (),
        (),
        (22102, 22110, 22125, 22010),
        (),
        (13022,),
        (),
        (),
        (22000,),
        (),
        (13045, 20170, 22023, 21023, 13065),
        (),
        (),
        (),
        (23102, 23110, 23122, 23130, 12045),
        (),
        (23003,),
        (),
        (23145, 23160, 23172, 23023, 20102),
        (),
        (),
        (),
        (23043, 22145, 22165, 23063, 20122),
        (22043,),
        (20112,),
        (),
        (21160, 21145, 22063, 21172, 21060, 20132, 20145, 30000, 30010, 21043, 20162, 30020, 21070, 30030,
         30040, 30050, 30070, 30060),
    ),
    (
        (11003, 11004, 11012, 11025, 11023, 11024, 11045, 10003, 12004, 10012, 10023, 12024, 10025, 11120,
         13005, 13004, 10111, 11065, 10043),
        (10123, 10121, 12005),
        (),
        (13024,),
        (13111, 10063, 13045, 11043),
        (10065, 13044),
        (13131,),
        (11063,),
        (),
        (12032,),
        (13064,),
        (),
        (23100, 12045, 12044, 10163, 23120, 12065, 12064),
        (),
        (20102,),
        (11044,),
        (22003, 22122),
        (22103,),
        (12164, 20122),
        (22030, 21122),
        (),
        (23172, 11064),
        (22020,),
        (22130,),
        (23112,),
        (11144, 22160),
        (23132,),
        (23143, 22145),
        (),
        (20172, 11164),
        (31020,),
        (23003,),
        (23162, 20111, 22172, 20131, 23023, 20161, 20145, 21105, 23043, 20004, 21132, 23063, 21145, 20024,
         22043, 20044, 21165, 31000, 31010, 31030, 20064, 22063, 31040, 31050, 31060, 31070),
    ),
)


def expert_weights(expert_ids, gate_nums, experts):
    gates = gate_nums.astype(jnp.float32) / denominator
    labels = jnp.arange(experts, dtype=jnp.int32)
    onehot = expert_ids[:, :, None] == labels[None, None, :]
    return jnp.sum(jnp.where(onehot, gates[:, :, None], 0.0), axis=1)


def digits(code):
    way = code % 10
    return code // 10000, code // 1000 % 10, code // 100 % 10, code // 10 % 10, 1 + way // 3, way % 3


def script(depth):
    tokens, results = [{} for _ in SENDS], [{} for _ in SENDS]
    for role, pieces in enumerate(SENDS):
        for kind, o, r, u, units, way in [digits(code) for piece in pieces for code in piece]:
            there, o, r, way = role + (way == AWAY) - (way == HOME), o, r ^ (way == ACROSS), way
            if there == depth // 2:
                there, o, way = role, depth - 1 - o, HOME
            for v in range(u, u + units):
                if kind == 1:
                    tokens[there][o, r, v] = (u, units)
                if kind == 2:
                    results[there].setdefault((o, r, v), []).append((way, u, units))
    acts = []
    for role, pieces in enumerate(SENDS):
        seen, heard, mine = set(), set(), []
        for index, piece in enumerate(pieces):
            found = []

            def need(o, r, u):
                if (o, r) != (role, 0) and (o, r, u) not in seen:
                    first, units = tokens[role][o, r, u]
                    seen.update((o, r, first + v) for v in range(units))
                    found.append((0, o, r, first, units, ACROSS, ()))

            for kind, o, r, u, units, way in [digits(code) for code in piece]:
                ways = []
                for v in range(u, u + units):
                    if kind == 1:
                        need(o, r, v)
                        continue
                    for source, first, size in results[role].get((o, r, v), []):
                        if (source, o, r, first) not in heard:
                            heard.add((source, o, r, first))
                            found.append((4, o, r, first, size, source, ()))
                    ways.append(tuple(source for source, _, _ in results[role].get((o, r, v), [])))
                found.append((kind, o, r, u, units, way, tuple(ways)))
            if index % PIECES == 0 and index < len(ROUNDS[role]) * PIECES:
                o, h = ROUNDS[role][index // PIECES]
                for r in range(SIDE):
                    for u in range(h * UNITS // 2, (h + 1) * UNITS // 2):
                        need(o, r, u)
            mine.append(found)
        acts.append(mine)
    return acts


def kernel(
    n, local,
    ids, nums, tokens, w_gate, w_up, w_down, out,
    rows, weights, factors, columns, gate, up, down, hidden, part, line, side,
    load_sem, weight_send, weight_recv, token_send, token_recv, result_send, line_recv, side_recv,
):
    depth = n // SIDE
    me = lax.axis_index("ep")
    z, y = me // SIDE, me % SIDE
    flip = z // (depth // 2)
    place = z + flip * (depth - 1 - 2 * z)
    count, width = tokens.shape
    ff = w_gate.shape[2]
    size = count // UNITS
    half = count // 2
    spots = depth * SIDE * UNITS
    acts = script(depth)
    steps = len(ROUNDS[0])

    def owner_of(o):
        return o + flip * (depth - 1 - 2 * o)

    def row_of(r):
        return y if r == 0 else 1 - y

    def offset(o, r, u):
        return owner_of(o) * SIDE * count + u * size // half * count + row_of(r) * half + u * size % half

    def spot(o, r, u):
        return (owner_of(o) * SIDE + row_of(r)) * UNITS + u

    def cut(start, extent=size):
        return pl.ds(pl.multiple_of(start, size), extent)

    def heading(way):
        return flip if way == AWAY else 1 - flip

    def device(way):
        return z * SIDE + 1 - y if way == ACROSS else me + SIDE * (1 - 2 * heading(way))

    def remote(source, target, send, recv, there):
        return pltpu.make_async_remote_copy(
            src_ref=source, dst_ref=target, send_sem=send, recv_sem=recv,
            device_id={"ep": there}, device_id_type=pl.DeviceIdType.MESH,
        )

    def token_copy(o, r, u, units, way):
        ref = rows.at[cut(offset(o, r, u), units * size)]
        return remote(ref, ref, token_send.at[way], token_recv.at[spot(o, r, u)], device(way))

    def landing(o, r, u, units, way):
        if way == ACROSS:
            start, recv = owner_of(o) * count + u * size, side_recv.at[owner_of(o) * UNITS + u]
            return side.at[cut(start, units * size)], recv
        start = heading(way) * (depth * SIDE * count) + offset(o, r, u)
        return line.at[cut(start, units * size)], line_recv.at[heading(way) * spots + spot(o, r, u)]

    def result_copy(o, r, u, units, way):
        target, recv = landing(o, r, u, units, way)
        source = part.at[cut(offset(o, r, u), units * size)]
        return remote(source, target, result_send.at[way], recv, device(way))

    own = []
    for h in range(2):
        start = z * SIDE * count + h * count + y * half
        own.append(
            pltpu.make_async_copy(tokens.at[pl.ds(h * half, half)], rows.at[cut(start, half)], load_sem.at[h])
        )
    loads = []
    for e in range(local):
        loads.append(pltpu.make_async_copy(w_gate.at[e], gate.at[e], load_sem.at[2 + 3 * e]))
        loads.append(pltpu.make_async_copy(w_up.at[e], up.at[e], load_sem.at[3 + 3 * e]))
    for e in range(local):
        loads.append(pltpu.make_async_copy(w_down.at[e], down.at[pl.ds(e * ff, ff)], load_sem.at[4 + 3 * e]))
    for load in own + loads:
        load.start()

    barrier = pltpu.get_barrier_semaphore()
    for k in range(1, n):
        pl.semaphore_signal(
            barrier, inc=1, device_id={"ep": (me + k) % n}, device_id_type=pl.DeviceIdType.MESH
        )

    gates = nums[...].astype(jnp.float32) / denominator
    for d in range(n):
        for e in range(local):
            chosen = jnp.where(ids[...] == d * local + e, gates, 0.0)
            weights[d, e : e + 1] = jnp.sum(chosen, axis=0, keepdims=True)
    factors[me] = weights[me]

    pl.semaphore_wait(barrier, n - 1)
    for load in own:
        load.wait()

    def added(o, r, u, units, ways):
        total = part[cut(offset(o, r, u), units * size)].astype(jnp.float32)
        for way in ways:
            total = total + landing(o, r, u, units, way)[0][...].astype(jnp.float32)
        return total

    def act(kind, o, r, u, units, way, ways):
        if kind == 0:
            token_copy(o, r, u, units, way).wait_recv()
        elif kind == 1:
            token_copy(o, r, u, units, way).start()
        elif kind == 4:
            target, recv = landing(o, r, u, units, way)
            remote(target, target, result_send.at[way], recv, device(way)).wait_recv()
        elif kind == 3:
            out[pl.ds(u * size, size)] = added(o, r, u, units, ways[0]).astype(out.dtype)
        else:
            together = units if len(set(ways)) == 1 else 1
            for v in range(0, units, together):
                if ways[v]:
                    total = added(o, r, u + v, together, ways[v])
                    part[cut(offset(o, r, u + v), together * size)] = total.astype(part.dtype)
            result_copy(o, r, u, units, way).start()

    def talk(p, i):
        for role, pieces in enumerate(acts):
            for step in range(steps):
                piece = pieces[step * PIECES + p]

                def body(piece=piece):
                    for action in piece:
                        act(*action)

                if piece:
                    pl.when((place == role) & (i == step))(body)

    def pick(i, which):
        found = jnp.int32(0)
        for role, rounds in enumerate(ROUNDS):
            for step, entry in enumerate(rounds):
                if entry[which]:
                    found = found + jnp.where((place == role) & (i == step), entry[which], 0)
        return found

    def weight_copy(k):
        there = (me + k) % n
        return remote(weights.at[there], factors.at[me], weight_send.at[0], weight_recv.at[me], there)

    for k in range(1, n):
        weight_copy(k).start()

    def ready():
        for k in range(1, n):
            source = (me + k) % n
            there = factors.at[source]
            remote(there, there, weight_send.at[0], weight_recv.at[source], source).wait_recv()
        for d in range(n):
            turned = jnp.concatenate([factors[d], jnp.zeros((-local % 8, count), jnp.float32)], axis=0).T
            for h in range(2):
                start = d // SIDE * SIDE * count + h * count + d % SIDE * half
                columns[pl.ds(start, half)] = turned[h * half : (h + 1) * half]

    def project(e, base):
        column = columns[cut(base, count), e : e + 1]

        def tile(t, carry):
            at = pl.ds(pl.multiple_of(t * LANES, LANES), LANES)
            block = rows[cut(base, count)]
            g = jnp.dot(block, gate[e, :, at], preferred_element_type=jnp.float32)
            v = jnp.dot(block, up[e, :, at], preferred_element_type=jnp.float32)
            h = g / (1.0 + jnp.exp(-g)) * v * column
            hidden[:, pl.ds(pl.multiple_of(e * ff + t * LANES, LANES), LANES)] = h.astype(jnp.bfloat16)
            return carry

        lax.fori_loop(0, ff // LANES, tile, 0, unroll=True)

    def spread(low, high, base):
        def tile(t, carry):
            at = pl.ds(pl.multiple_of(t * LANES, LANES), LANES)
            result = jnp.dot(hidden[...], down[:, at], preferred_element_type=jnp.float32)
            part[cut(base, count), at] = result.astype(jnp.bfloat16)
            return carry

        lax.fori_loop(low, high, tile, 0, unroll=True)

    def step(i, carry):
        o, h = pick(i, 0), pick(i, 1)
        base = owner_of(o) * SIDE * count + h * count
        tiles = width // LANES
        for p in range(PIECES):
            talk(p, i)

            @pl.when(i == 0)
            def _():
                if p == 0:
                    ready()
                for load in loads[2 * p : 2 * p + 2] if p < local else loads[2 * local :] if p == local else []:
                    load.wait()

            if p < local:
                project(p, base)
            else:
                share = tiles // (PIECES - local)
                spread((p - local) * share, (p - local + 1) * share, base)
        return carry

    lax.fori_loop(0, steps, step, 0)

    def ending(role):
        for piece in acts[role][steps * PIECES :]:
            for action in piece:
                act(*action)
        for way in (AWAY, HOME, ACROSS):
            for kind, sems in ((1, token_send), (2, result_send)):
                sent = sum(a[4] for piece in acts[role] for a in piece if a[0] == kind and a[5] == way)
                if sent:
                    all_of = rows.at[pl.ds(0, sent * size)]
                    remote(all_of, all_of, sems.at[way], token_recv.at[0], device(way)).wait_send()

    for role in range(len(acts)):
        pl.when(place == role)(functools.partial(ending, role))
    given = weights.at[pl.ds(0, n - 1)]
    remote(given, given, weight_send.at[0], weight_recv.at[0], device(ACROSS)).wait_send()


def fused(tokens, expert_ids, gate_nums, w_gate, w_up, w_down, n):
    count, width = tokens.shape
    local, _, ff = w_gate.shape
    depth = n // SIDE
    everyone = n * count
    kind = tokens.dtype
    dma = pltpu.SemaphoreType.DMA
    vmem = pl.BlockSpec(memory_space=pltpu.VMEM)
    hbm = pl.BlockSpec(memory_space=pl.ANY)
    return pl.pallas_call(
        functools.partial(kernel, n, local),
        out_shape=jax.ShapeDtypeStruct((count, width), kind),
        in_specs=[vmem, vmem, hbm, hbm, hbm, hbm],
        out_specs=vmem,
        scratch_shapes=[
            pltpu.VMEM((everyone, width), kind),
            pltpu.VMEM((n, local, count), jnp.float32),
            pltpu.VMEM((n, local, count), jnp.float32),
            pltpu.VMEM((everyone, local + -local % 8), jnp.float32),
            pltpu.VMEM((local, width, ff), kind),
            pltpu.VMEM((local, width, ff), kind),
            pltpu.VMEM((local * ff, width), kind),
            pltpu.VMEM((count, local * ff), kind),
            pltpu.VMEM((everyone, width), kind),
            pltpu.VMEM((2 * everyone, width), kind),
            pltpu.VMEM((depth * count, width), kind),
            dma((2 + 3 * local,)),
            dma((1,)), dma((n,)),
            dma((3,)), dma((n * UNITS,)),
            dma((3,)), dma((2 * n * UNITS,)), dma((depth * UNITS,)),
        ],
        compiler_params=pltpu.CompilerParams(
            collective_id=0, has_side_effects=True, vmem_limit_bytes=VMEM
        ),
    )(expert_ids.T, gate_nums.T, tokens, w_gate, w_up, w_down)


def plain(tokens, expert_ids, gate_nums, w_gate, w_up, w_down, n):
    weight = expert_weights(expert_ids, gate_nums, w_gate.shape[0] * n)
    weights = lax.all_to_all(weight, "ep", split_axis=1, concat_axis=0, tiled=True)
    rows = lax.all_gather(tokens, "ep", axis=0, tiled=True)
    gate = jnp.einsum("td,xdf->xtf", rows, w_gate, preferred_element_type=jnp.float32)
    up = jnp.einsum("td,xdf->xtf", rows, w_up, preferred_element_type=jnp.float32)
    hidden = (jax.nn.silu(gate) * up * weights.T[:, :, None]).astype(jnp.bfloat16)
    result = jnp.einsum("xtf,xfd->td", hidden, w_down, preferred_element_type=jnp.float32)
    return lax.psum_scatter(
        result.astype(jnp.bfloat16), "ep", scatter_dimension=0, tiled=True
    )


def shards(n, tokens, expert_ids, gate_nums, w_gate, w_up, w_down):
    count, width = tokens.shape
    local, _, ff = w_gate.shape
    held = 5 * n * count * width + 3 * local * width * ff + 2 * count * local * ff
    fits = 2 * held < VMEM - 4 * 2**20
    planned = n == 2 * SIDE * len(SENDS) and PIECES == local + 2
    shaped = count % (16 * UNITS) == 0 and count % 128 == 0 and ff % LANES == 0 and width % (2 * LANES) == 0
    plan = fused if fits and planned and shaped else plain
    return plan(tokens, expert_ids, gate_nums, w_gate, w_up, w_down, n)


def solution(mesh):
    placed = (
        P(("dp", "ep"), None),
        P(("dp", "ep"), None),
        P(("dp", "ep"), None),
        P("ep", None, None),
        P("ep", None, None),
        P("ep", None, None),
    )
    return jax.shard_map(
        functools.partial(shards, mesh.shape["ep"]),
        mesh=mesh, in_specs=placed, out_specs=P(("dp", "ep"), None), check_vma=False,
    )
```

```python
import functools

import jax
import jax.numpy as jnp
from jax import lax
from jax.experimental import pallas as pl
from jax.experimental.pallas import tpu as pltpu
from jax.sharding import PartitionSpec as P

denominator = 1024.0
SIDE = 2
LANES = 256
VMEM = 53 * 2**20

AWAY, HOME, ACROSS = 0, 1, 2
UNITS = 8
PIECES = 4
ROUNDS = (
    ((1, 0), (2, 0), (0, 0), (0, 1), (3, 0), (3, 1), (2, 1), (1, 1)),
    ((0, 0), (1, 0), (3, 0), (2, 0), (3, 1), (2, 1), (0, 1), (1, 1)),
)
SENDS = (
    (
        (50000, 10003, 10002, 10032, 10023, 10045, 10100, 10043, 51000, 11005, 11025, 10143, 52000, 10063,
         12005, 11100, 53000, 12025),
        (),
        (),
        (),
        (21122, 21103, 21130, 10065, 13002, 21003),
        (),
        (),
        (),
        (),
        (22102, 22110, 22125, 22010),
        (),
        (13022,),
        (),
        (),
        (22000,),
        (),
        (13045, 20170, 22023, 21023, 13065),
        (),
        (),
        (),
        (23102, 23110, 23122, 23130, 12045),
        (),
        (23003,),
        (),
        (23145, 23160, 23172, 23023, 20102),
        (),
        (),
        (),
        (23043, 22145, 22165, 23063, 20122),
        (22043,),
        (20112,),
        (),
        (21160, 21145, 22063, 21172, 21060, 20132, 20145, 30000, 30010, 21043, 20162, 30020, 21070, 30030,
         30040, 30050, 30070, 30060),
    ),
    (
        (51000, 11003, 11004, 11012, 11025, 11023, 11024, 11045, 50000, 52000, 10003, 12004, 10012, 10023,
         12024, 10025, 11120, 53000, 13005, 13004, 10111, 11065, 10043),
        (10123, 10121, 12005),
        (),
        (13024,),
        (13111, 10063, 13045, 11043),
        (10065, 13044),
        (13131,),
        (11063,),
        (),
        (12032,),
        (13064,),
        (),
        (23100, 12045, 12044, 10163, 23120, 12065, 12064),
        (),
        (20102,),
        (11044,),
        (22003, 22122),
        (22103,),
        (12164, 20122),
        (22030, 21122),
        (),
        (23172, 11064),
        (22020,),
        (22130,),
        (23112,),
        (11144, 22160),
        (23132,),
        (23143, 22145),
        (),
        (20172, 11164),
        (31020,),
        (23003,),
        (23162, 20111, 22172, 20131, 23023, 20161, 20145, 21105, 23043, 20004, 21132, 23063, 21145, 20024,
         22043, 20044, 21165, 31000, 31010, 31030, 20064, 22063, 31040, 31050, 31060, 31070),
    ),
)


def expert_weights(expert_ids, gate_nums, experts):
    gates = gate_nums.astype(jnp.float32) / denominator
    labels = jnp.arange(experts, dtype=jnp.int32)
    onehot = expert_ids[:, :, None] == labels[None, None, :]
    return jnp.sum(jnp.where(onehot, gates[:, :, None], 0.0), axis=1)


def digits(code):
    way = code % 10
    return code // 10000, code // 1000 % 10, code // 100 % 10, code // 10 % 10, 1 + way // 3, way % 3


def script(depth):
    tokens, results = [{} for _ in SENDS], [{} for _ in SENDS]
    for role, pieces in enumerate(SENDS):
        for kind, o, r, u, units, way in [digits(code) for piece in pieces for code in piece]:
            there, o, r, way = role + (way == AWAY) - (way == HOME), o, r ^ (way == ACROSS), way
            if there == depth // 2:
                there, o, way = role, depth - 1 - o, HOME
            for v in range(u, u + units):
                if kind == 1:
                    tokens[there][o, r, v] = (u, units)
                if kind == 2:
                    results[there].setdefault((o, r, v), []).append((way, u, units))
    acts = []
    for role, pieces in enumerate(SENDS):
        seen, heard, mine = set(), set(), []
        for index, piece in enumerate(pieces):
            found = []

            def need(o, r, u):
                if (o, r) != (role, 0) and (o, r, u) not in seen:
                    first, units = tokens[role][o, r, u]
                    seen.update((o, r, first + v) for v in range(units))
                    found.append((0, o, r, first, units, ACROSS, ()))

            for kind, o, r, u, units, way in [digits(code) for code in piece]:
                ways = []
                for v in range(u, u + units):
                    if kind == 1:
                        need(o, r, v)
                    if kind not in (2, 3):
                        continue
                    for source, first, size in results[role].get((o, r, v), []):
                        if (source, o, r, first) not in heard:
                            heard.add((source, o, r, first))
                            found.append((4, o, r, first, size, source, ()))
                    ways.append(tuple(source for source, _, _ in results[role].get((o, r, v), [])))
                found.append((kind, o, r, u, units, way, tuple(ways)))
            if index % PIECES == 0 and index < len(ROUNDS[role]) * PIECES:
                o, h = ROUNDS[role][index // PIECES]
                if o not in [entry[0] for entry in ROUNDS[role][: index // PIECES]]:
                    found.append((6, o, 0, 0, 0, 0, ()))
                for r in range(SIDE):
                    for u in range(h * UNITS // 2, (h + 1) * UNITS // 2):
                        need(o, r, u)
            mine.append(found)
        acts.append(mine)
    return acts


def kernel(
    n, local,
    ids, nums, tokens, w_gate, w_up, w_down, out,
    rows, shares, factors, columns, gate, up, down, hidden, part, line, side,
    load_sem, share_send, share_recv, factor_send, factor_recv, token_send, token_recv, result_send, line_recv, side_recv,
):
    depth = n // SIDE
    me = lax.axis_index("ep")
    z, y = me // SIDE, me % SIDE
    flip = z // (depth // 2)
    place = z + flip * (depth - 1 - 2 * z)
    count, width = tokens.shape
    ff = w_gate.shape[2]
    size = count // UNITS
    half = count // 2
    spots = depth * SIDE * UNITS
    acts = script(depth)
    steps = len(ROUNDS[0])

    def owner_of(o):
        return o + flip * (depth - 1 - 2 * o)

    def row_of(r):
        return y if r == 0 else 1 - y

    def offset(o, r, u):
        return owner_of(o) * SIDE * count + u * size // half * count + row_of(r) * half + u * size % half

    def spot(o, r, u):
        return (owner_of(o) * SIDE + row_of(r)) * UNITS + u

    def cut(start, extent=size):
        return pl.ds(pl.multiple_of(start, size), extent)

    def heading(way):
        return flip if way == AWAY else 1 - flip

    def device(way):
        return z * SIDE + 1 - y if way == ACROSS else me + SIDE * (1 - 2 * heading(way))

    def remote(source, target, send, recv, there):
        return pltpu.make_async_remote_copy(
            src_ref=source, dst_ref=target, send_sem=send, recv_sem=recv,
            device_id={"ep": there}, device_id_type=pl.DeviceIdType.MESH,
        )

    def token_copy(o, r, u, units, way):
        ref = rows.at[cut(offset(o, r, u), units * size)]
        return remote(ref, ref, token_send.at[way], token_recv.at[spot(o, r, u)], device(way))

    def landing(o, r, u, units, way):
        if way == ACROSS:
            start, recv = owner_of(o) * count + u * size, side_recv.at[owner_of(o) * UNITS + u]
            return side.at[cut(start, units * size)], recv
        start = heading(way) * (depth * SIDE * count) + offset(o, r, u)
        return line.at[cut(start, units * size)], line_recv.at[heading(way) * spots + spot(o, r, u)]

    def result_copy(o, r, u, units, way):
        target, recv = landing(o, r, u, units, way)
        source = part.at[cut(offset(o, r, u), units * size)]
        return remote(source, target, result_send.at[way], recv, device(way))

    own = []
    for h in range(2):
        start = z * SIDE * count + h * count + y * half
        own.append(
            pltpu.make_async_copy(tokens.at[pl.ds(h * half, half)], rows.at[cut(start, half)], load_sem.at[h])
        )
    loads = []
    for e in range(local):
        loads.append(pltpu.make_async_copy(w_gate.at[e], gate.at[e], load_sem.at[2 + 3 * e]))
        loads.append(pltpu.make_async_copy(w_up.at[e], up.at[e], load_sem.at[3 + 3 * e]))
    for e in range(local):
        loads.append(pltpu.make_async_copy(w_down.at[e], down.at[pl.ds(e * ff, ff)], load_sem.at[4 + 3 * e]))
    for load in own + loads:
        load.start()

    barrier = pltpu.get_barrier_semaphore()
    def greet(there):
        pl.semaphore_signal(barrier, inc=1, device_id={"ep": there}, device_id_type=pl.DeviceIdType.MESH)

    greet(device(ACROSS))
    greet(device(AWAY))
    pl.when(place > 0)(lambda: greet(device(HOME)))

    gates = nums[...].astype(jnp.float32) / denominator
    for d in range(n):
        for e in range(local):
            chosen = jnp.where(ids[...] == d * local + e, gates, 0.0)
            shares[z * n + d, e : e + 1] = jnp.sum(chosen, axis=0, keepdims=True)

    pl.when(place == 0)(lambda: pl.semaphore_wait(barrier, 2))
    pl.when(place > 0)(lambda: pl.semaphore_wait(barrier, 3))
    for load in own:
        load.wait()

    def added(o, r, u, units, ways):
        total = part[cut(offset(o, r, u), units * size)].astype(jnp.float32)
        for way in ways:
            total = total + landing(o, r, u, units, way)[0][...].astype(jnp.float32)
        return total

    def onward(role, o):
        return [AWAY] * (o <= role) + [HOME] * (o >= role and role > 0)

    def beyond(role, way):
        return SIDE * (depth - 1 - role if way == AWAY else role)

    def share_copy(role, o, way):
        first = SIDE * (z + 1) if way == AWAY else 0
        mirrored = 0 if way == AWAY else SIDE * (z + 1)
        ref = shares.at[pl.ds(owner_of(o) * n + jnp.where(flip == 0, first, mirrored), beyond(role, way))]
        return remote(ref, ref, share_send.at[0], share_recv.at[owner_of(o)], device(way))

    def factor_copy(o):
        there = device(ACROSS)
        return remote(
            shares.at[owner_of(o) * n + there], factors.at[owner_of(o)], factor_send.at[0], factor_recv.at[owner_of(o)], there
        )

    def pass_on(role, o):
        if o != role:
            extent = SIDE * (depth - role if o < role else role + 1)
            start = jnp.where((flip == 0) == (o < role), SIDE * z, 0)
            ref = shares.at[pl.ds(owner_of(o) * n + start, extent)]
            remote(ref, ref, share_send.at[0], share_recv.at[owner_of(o)], device(ACROSS)).wait_recv()
        for way in onward(role, o):
            share_copy(role, o, way).start()
        factor_copy(o).start()

    def lay_out(o):
        factor_copy(o).wait_recv()
        for r, block in ((0, shares[owner_of(o) * n + me]), (1, factors[owner_of(o)])):
            turned = jnp.concatenate([block, jnp.zeros((-local % 8, count), jnp.float32)], axis=0).T
            for h in range(2):
                start = owner_of(o) * SIDE * count + h * count + row_of(r) * half
                columns[cut(start, half)] = turned[h * half : (h + 1) * half]

    def act(role, kind, o, r, u, units, way, ways):
        if kind == 0:
            token_copy(o, r, u, units, way).wait_recv()
        elif kind == 1:
            token_copy(o, r, u, units, way).start()
        elif kind == 4:
            target, recv = landing(o, r, u, units, way)
            remote(target, target, result_send.at[way], recv, device(way)).wait_recv()
        elif kind == 5:
            pass_on(role, o)
        elif kind == 6:
            lay_out(o)
        elif kind == 3:
            out[pl.ds(u * size, size)] = added(o, r, u, units, ways[0]).astype(out.dtype)
        else:
            together = units if len(set(ways)) == 1 else 1
            for v in range(0, units, together):
                if ways[v]:
                    total = added(o, r, u + v, together, ways[v])
                    part[cut(offset(o, r, u + v), together * size)] = total.astype(part.dtype)
            result_copy(o, r, u, units, way).start()

    def talk(p, i):
        for role, pieces in enumerate(acts):
            for step in range(steps):
                piece = pieces[step * PIECES + p]

                def body(role=role, piece=piece):
                    for action in piece:
                        act(role, *action)

                if piece:
                    pl.when((place == role) & (i == step))(body)

    def pick(i, which):
        found = jnp.int32(0)
        for role, rounds in enumerate(ROUNDS):
            for step, entry in enumerate(rounds):
                if entry[which]:
                    found = found + jnp.where((place == role) & (i == step), entry[which], 0)
        return found

    def project(e, base):
        column = columns[cut(base, count), e : e + 1]

        def tile(t, carry):
            at = pl.ds(pl.multiple_of(t * LANES, LANES), LANES)
            block = rows[cut(base, count)]
            g = jnp.dot(block, gate[e, :, at], preferred_element_type=jnp.float32)
            v = jnp.dot(block, up[e, :, at], preferred_element_type=jnp.float32)
            h = g / (1.0 + jnp.exp(-g)) * v * column
            hidden[:, pl.ds(pl.multiple_of(e * ff + t * LANES, LANES), LANES)] = h.astype(jnp.bfloat16)
            return carry

        lax.fori_loop(0, ff // LANES, tile, 0, unroll=True)

    def spread(low, high, base):
        def tile(t, carry):
            at = pl.ds(pl.multiple_of(t * LANES, LANES), LANES)
            result = jnp.dot(hidden[...], down[:, at], preferred_element_type=jnp.float32)
            part[cut(base, count), at] = result.astype(jnp.bfloat16)
            return carry

        lax.fori_loop(low, high, tile, 0, unroll=True)

    def step(i, carry):
        o, h = pick(i, 0), pick(i, 1)
        base = owner_of(o) * SIDE * count + h * count
        tiles = width // LANES
        for p in range(PIECES):
            talk(p, i)

            @pl.when(i == 0)
            def _():
                for load in loads[2 * p : 2 * p + 2] if p < local else loads[2 * local :] if p == local else []:
                    load.wait()

            if p < local:
                project(p, base)
            else:
                share = tiles // (PIECES - local)
                spread((p - local) * share, (p - local + 1) * share, base)
        return carry

    lax.fori_loop(0, steps, step, 0)

    def ending(role):
        for piece in acts[role][steps * PIECES :]:
            for action in piece:
                act(role, *action)
        for way in (AWAY, HOME, ACROSS):
            for kind, sems in ((1, token_send), (2, result_send)):
                sent = sum(a[4] for piece in acts[role] for a in piece if a[0] == kind and a[5] == way)
                if sent:
                    all_of = rows.at[pl.ds(0, sent * size)]
                    remote(all_of, all_of, sems.at[way], token_recv.at[0], device(way)).wait_send()

        passed = sum(beyond(role, way) for o in range(depth) for way in onward(role, o))
        given = shares.at[pl.ds(0, passed)]
        remote(given, given, share_send.at[0], share_recv.at[0], device(ACROSS)).wait_send()

    for role in range(len(acts)):
        pl.when(place == role)(functools.partial(ending, role))
    remote(factors, factors, factor_send.at[0], factor_recv.at[0], device(ACROSS)).wait_send()


def fused(tokens, expert_ids, gate_nums, w_gate, w_up, w_down, n):
    count, width = tokens.shape
    local, _, ff = w_gate.shape
    depth = n // SIDE
    everyone = n * count
    kind = tokens.dtype
    dma = pltpu.SemaphoreType.DMA
    vmem = pl.BlockSpec(memory_space=pltpu.VMEM)
    hbm = pl.BlockSpec(memory_space=pl.ANY)
    return pl.pallas_call(
        functools.partial(kernel, n, local),
        out_shape=jax.ShapeDtypeStruct((count, width), kind),
        in_specs=[vmem, vmem, hbm, hbm, hbm, hbm],
        out_specs=vmem,
        scratch_shapes=[
            pltpu.VMEM((everyone, width), kind),
            pltpu.VMEM((depth * n, local, count), jnp.float32),
            pltpu.VMEM((depth, local, count), jnp.float32),
            pltpu.VMEM((everyone, local + -local % 8), jnp.float32),
            pltpu.VMEM((local, width, ff), kind),
            pltpu.VMEM((local, width, ff), kind),
            pltpu.VMEM((local * ff, width), kind),
            pltpu.VMEM((count, local * ff), kind),
            pltpu.VMEM((everyone, width), kind),
            pltpu.VMEM((2 * everyone, width), kind),
            pltpu.VMEM((depth * count, width), kind),
            dma((2 + 3 * local,)),
            dma((1,)), dma((depth,)), dma((1,)), dma((depth,)),
            dma((3,)), dma((n * UNITS,)),
            dma((3,)), dma((2 * n * UNITS,)), dma((depth * UNITS,)),
        ],
        compiler_params=pltpu.CompilerParams(
            collective_id=0, has_side_effects=True, vmem_limit_bytes=VMEM
        ),
    )(expert_ids.T, gate_nums.T, tokens, w_gate, w_up, w_down)


def plain(tokens, expert_ids, gate_nums, w_gate, w_up, w_down, n):
    weight = expert_weights(expert_ids, gate_nums, w_gate.shape[0] * n)
    weights = lax.all_to_all(weight, "ep", split_axis=1, concat_axis=0, tiled=True)
    rows = lax.all_gather(tokens, "ep", axis=0, tiled=True)
    gate = jnp.einsum("td,xdf->xtf", rows, w_gate, preferred_element_type=jnp.float32)
    up = jnp.einsum("td,xdf->xtf", rows, w_up, preferred_element_type=jnp.float32)
    hidden = (jax.nn.silu(gate) * up * weights.T[:, :, None]).astype(jnp.bfloat16)
    result = jnp.einsum("xtf,xfd->td", hidden, w_down, preferred_element_type=jnp.float32)
    return lax.psum_scatter(
        result.astype(jnp.bfloat16), "ep", scatter_dimension=0, tiled=True
    )


def shards(n, tokens, expert_ids, gate_nums, w_gate, w_up, w_down):
    count, width = tokens.shape
    local, _, ff = w_gate.shape
    held = 5 * n * count * width + 3 * local * width * ff + 2 * count * local * ff
    fits = 2 * held < VMEM - 4 * 2**20
    planned = n == 2 * SIDE * len(SENDS) and PIECES == local + 2
    shaped = count % (16 * UNITS) == 0 and count % 128 == 0 and ff % LANES == 0 and width % (2 * LANES) == 0
    plan = fused if fits and planned and shaped else plain
    return plan(tokens, expert_ids, gate_nums, w_gate, w_up, w_down, n)


def solution(mesh):
    placed = (
        P(("dp", "ep"), None),
        P(("dp", "ep"), None),
        P(("dp", "ep"), None),
        P("ep", None, None),
        P("ep", None, None),
        P("ep", None, None),
    )
    return jax.shard_map(
        functools.partial(shards, mesh.shape["ep"]),
        mesh=mesh, in_specs=placed, out_specs=P(("dp", "ep"), None), check_vma=False,
    )
```

```python
import functools

import jax
import jax.numpy as jnp
from jax import lax
from jax.experimental import pallas as pl
from jax.experimental.pallas import tpu as pltpu
from jax.sharding import PartitionSpec as P

denominator = 1024.0
SIDE = 2
LANES = 256
VMEM = 53 * 2**20

AWAY, HOME, ACROSS = 0, 1, 2
UNITS = 8
PIECES = 4
ROUNDS = (
    ((1, 0), (2, 0), (0, 0), (0, 1), (3, 0), (3, 1), (2, 1), (1, 1)),
    ((0, 0), (1, 0), (3, 0), (2, 0), (3, 1), (2, 1), (0, 1), (1, 1)),
)
SENDS = (
    (
        (500010, 100020, 100012, 100312, 100220, 100422, 101010, 100420, 510010, 110022, 110222, 101420,
         520010, 100620, 120022, 111010, 530010, 120222),
        (),
        (),
        (),
        (211212, 211020, 211310, 100622, 130012, 210020),
        (),
        (),
        (),
        (),
        (221012, 221110, 221222, 220110),
        (),
        (130212,),
        (),
        (),
        (220010,),
        (),
        (130422, 201710, 220220, 210220, 130622),
        (),
        (),
        (),
        (231012, 231110, 231212, 231310, 120422),
        (),
        (230020,),
        (),
        (231422, 231610, 231712, 230220, 201012),
        (),
        (),
        (),
        (230420, 221422, 221622, 230620, 201212),
        (220420,),
        (201112,),
        (),
        (211610, 211422, 220620, 211712, 210610, 201312, 201422, 300010, 300110, 210420, 201612, 300210,
         210710, 300310, 300410, 300510, 300710, 300610),
    ),
    (
        (510010, 110020, 110021, 110112, 110222, 110220, 110221, 110422, 500010, 520010, 100020, 120021,
         100112, 100220, 120221, 100222, 111210, 530010, 130022, 130021, 101111, 110622, 100420),
        (101220, 101211, 120022),
        (),
        (130221,),
        (131111, 100620, 130422, 110420),
        (100622, 130421),
        (131311,),
        (110620,),
        (),
        (120312,),
        (130621,),
        (),
        (231010, 120422, 120421, 101620, 231210, 120622, 120621),
        (),
        (201012,),
        (110421,),
        (220020, 221212),
        (221020,),
        (121621, 201212),
        (220310, 211212),
        (),
        (231712, 110621),
        (220210,),
        (221310,),
        (231112,),
        (111421, 221610),
        (231312,),
        (231420, 221422),
        (),
        (201712, 111621),
        (310210,),
        (230020,),
        (231612, 201111, 221712, 201311, 230220, 201611, 201422, 211022, 230420, 200021, 211312, 230620,
         211422, 200221, 220420, 200421, 211622, 310010, 310110, 310310, 200621, 220620, 310410, 310510,
         310610, 310710),
    ),
)


def expert_weights(expert_ids, gate_nums, experts):
    gates = gate_nums.astype(jnp.float32) / denominator
    labels = jnp.arange(experts, dtype=jnp.int32)
    onehot = expert_ids[:, :, None] == labels[None, None, :]
    return jnp.sum(jnp.where(onehot, gates[:, :, None], 0.0), axis=1)


def digits(code):
    return tuple(code // 10**k % 10 for k in range(5, -1, -1))


def script(depth):
    tokens, results = [{} for _ in SENDS], [{} for _ in SENDS]
    for role, pieces in enumerate(SENDS):
        for kind, o, r, u, units, way in [digits(code) for piece in pieces for code in piece]:
            there, o, r, way = role + (way == AWAY) - (way == HOME), o, r ^ (way == ACROSS), way
            if there == depth // 2:
                there, o, way = role, depth - 1 - o, HOME
            for v in range(u, u + units):
                if kind == 1:
                    tokens[there][o, r, v] = (u, units)
                if kind == 2:
                    results[there].setdefault((o, r, v), []).append((way, u, units))
    acts = []
    for role, pieces in enumerate(SENDS):
        seen, heard, mine = set(), set(), []
        for index, piece in enumerate(pieces):
            found = []

            def need(o, r, u):
                if (o, r) != (role, 0) and (o, r, u) not in seen:
                    first, units = tokens[role][o, r, u]
                    seen.update((o, r, first + v) for v in range(units))
                    found.append((0, o, r, first, units, ACROSS, ()))

            for kind, o, r, u, units, way in [digits(code) for code in piece]:
                ways = []
                for v in range(u, u + units):
                    if kind == 1:
                        need(o, r, v)
                    if kind not in (2, 3):
                        continue
                    for source, first, size in results[role].get((o, r, v), []):
                        if (source, o, r, first) not in heard:
                            heard.add((source, o, r, first))
                            found.append((4, o, r, first, size, source, ()))
                    ways.append(tuple(source for source, _, _ in results[role].get((o, r, v), [])))
                found.append((kind, o, r, u, units, way, tuple(ways)))
            if index % PIECES == 0 and index < len(ROUNDS[role]) * PIECES:
                o, h = ROUNDS[role][index // PIECES]
                if o not in [entry[0] for entry in ROUNDS[role][: index // PIECES]]:
                    found.append((6, o, 0, 0, 0, 0, ()))
                for r in range(SIDE):
                    for u in range(h * UNITS // 2, (h + 1) * UNITS // 2):
                        need(o, r, u)
            mine.append(found)
        acts.append(mine)
    return acts


def kernel(
    n, local,
    choices, tokens, w_gate, w_up, w_down, out,
    rows, shares, factors, columns, gate, up, down, hidden, part, line, side,
    load_sem, share_send, share_recv, factor_send, factor_recv, token_send, token_recv, result_send, line_recv, side_recv,
):
    depth = n // SIDE
    me = lax.axis_index("ep")
    z, y = me // SIDE, me % SIDE
    flip = z // (depth // 2)
    place = z + flip * (depth - 1 - 2 * z)
    count, width = tokens.shape
    ff = w_gate.shape[2]
    size = count // UNITS
    half = count // 2
    spots = depth * SIDE * UNITS
    acts = script(depth)
    steps = len(ROUNDS[0])

    def owner_of(o):
        return o + flip * (depth - 1 - 2 * o)

    def row_of(r):
        return y if r == 0 else 1 - y

    def offset(o, r, u):
        return owner_of(o) * SIDE * count + u * size // half * count + row_of(r) * half + u * size % half

    def spot(o, r, u):
        return (owner_of(o) * SIDE + row_of(r)) * UNITS + u

    def cut(start, extent=size):
        return pl.ds(pl.multiple_of(start, size), extent)

    def heading(way):
        return flip if way == AWAY else 1 - flip

    def device(way):
        return z * SIDE + 1 - y if way == ACROSS else me + SIDE * (1 - 2 * heading(way))

    def remote(source, target, send, recv, there):
        return pltpu.make_async_remote_copy(
            src_ref=source, dst_ref=target, send_sem=send, recv_sem=recv,
            device_id={"ep": there}, device_id_type=pl.DeviceIdType.MESH,
        )

    def token_copy(o, r, u, units, way):
        ref = rows.at[cut(offset(o, r, u), units * size)]
        return remote(ref, ref, token_send.at[way], token_recv.at[spot(o, r, u)], device(way))

    def landing(o, r, u, units, way):
        if way == ACROSS:
            start, recv = owner_of(o) * count + u * size, side_recv.at[owner_of(o) * UNITS + u]
            return side.at[cut(start, units * size)], recv
        start = heading(way) * (depth * SIDE * count) + offset(o, r, u)
        return line.at[cut(start, units * size)], line_recv.at[heading(way) * spots + spot(o, r, u)]

    def result_copy(o, r, u, units, way):
        target, recv = landing(o, r, u, units, way)
        source = part.at[cut(offset(o, r, u), units * size)]
        return remote(source, target, result_send.at[way], recv, device(way))

    barrier = pltpu.get_barrier_semaphore()
    def greet(there):
        pl.semaphore_signal(barrier, inc=1, device_id={"ep": there}, device_id_type=pl.DeviceIdType.MESH)

    greet(device(ACROSS))
    greet(device(AWAY))
    pl.when(place > 0)(lambda: greet(device(HOME)))

    own = []
    for h in range(2):
        start = z * SIDE * count + h * count + y * half
        own.append(
            pltpu.make_async_copy(tokens.at[pl.ds(h * half, half)], rows.at[cut(start, half)], load_sem.at[h])
        )
    loads = []
    for e in range(local):
        loads.append(pltpu.make_async_copy(w_gate.at[e], gate.at[e], load_sem.at[2 + 3 * e]))
        loads.append(pltpu.make_async_copy(w_up.at[e], up.at[e], load_sem.at[3 + 3 * e]))
    for e in range(local):
        loads.append(pltpu.make_async_copy(w_down.at[e], down.at[pl.ds(e * ff, ff)], load_sem.at[4 + 3 * e]))
    for load in own + loads:
        load.start()

    ids = choices[...] // int(denominator)
    gates = (choices[...] % int(denominator)).astype(jnp.float32) / denominator
    for d in range(n):
        for e in range(local):
            chosen = jnp.where(ids == d * local + e, gates, 0.0)
            shares[z * n + d, e : e + 1] = jnp.sum(chosen, axis=0, keepdims=True)

    pl.when(place == 0)(lambda: pl.semaphore_wait(barrier, 2))
    pl.when(place > 0)(lambda: pl.semaphore_wait(barrier, 3))
    for load in own:
        load.wait()

    def added(o, r, u, units, ways):
        total = part[cut(offset(o, r, u), units * size)].astype(jnp.float32)
        for way in ways:
            total = total + landing(o, r, u, units, way)[0][...].astype(jnp.float32)
        return total

    def onward(role, o):
        return [AWAY] * (o <= role) + [HOME] * (o >= role and role > 0)

    def beyond(role, way):
        return SIDE * (depth - 1 - role if way == AWAY else role)

    def share_copy(role, o, way):
        first = SIDE * (z + 1) if way == AWAY else 0
        mirrored = 0 if way == AWAY else SIDE * (z + 1)
        ref = shares.at[pl.ds(owner_of(o) * n + jnp.where(flip == 0, first, mirrored), beyond(role, way))]
        return remote(ref, ref, share_send.at[0], share_recv.at[owner_of(o)], device(way))

    def factor_copy(o):
        there = device(ACROSS)
        return remote(
            shares.at[owner_of(o) * n + there], factors.at[owner_of(o)], factor_send.at[0], factor_recv.at[owner_of(o)], there
        )

    def pass_on(role, o):
        if o != role:
            extent = SIDE * (depth - role if o < role else role + 1)
            start = jnp.where((flip == 0) == (o < role), SIDE * z, 0)
            ref = shares.at[pl.ds(owner_of(o) * n + start, extent)]
            remote(ref, ref, share_send.at[0], share_recv.at[owner_of(o)], device(ACROSS)).wait_recv()
        for way in onward(role, o):
            share_copy(role, o, way).start()
        factor_copy(o).start()

    def lay_out(o):
        factor_copy(o).wait_recv()
        for r, block in ((0, shares[owner_of(o) * n + me]), (1, factors[owner_of(o)])):
            turned = jnp.concatenate([block, jnp.zeros((-local % 8, count), jnp.float32)], axis=0).T
            for h in range(2):
                start = owner_of(o) * SIDE * count + h * count + row_of(r) * half
                columns[cut(start, half)] = turned[h * half : (h + 1) * half]

    def act(role, kind, o, r, u, units, way, ways):
        if kind == 0:
            token_copy(o, r, u, units, way).wait_recv()
        elif kind == 1:
            token_copy(o, r, u, units, way).start()
        elif kind == 4:
            target, recv = landing(o, r, u, units, way)
            remote(target, target, result_send.at[way], recv, device(way)).wait_recv()
        elif kind == 5:
            pass_on(role, o)
        elif kind == 6:
            lay_out(o)
        elif kind == 3:
            out[pl.ds(u * size, size)] = added(o, r, u, units, ways[0]).astype(out.dtype)
        else:
            together = units if len(set(ways)) == 1 else 1
            for v in range(0, units, together):
                if ways[v]:
                    total = added(o, r, u + v, together, ways[v])
                    part[cut(offset(o, r, u + v), together * size)] = total.astype(part.dtype)
            result_copy(o, r, u, units, way).start()

    def talk(p, i):
        for role, pieces in enumerate(acts):
            for step in range(steps):
                piece = pieces[step * PIECES + p]

                def body(role=role, piece=piece):
                    for action in piece:
                        act(role, *action)

                if piece:
                    pl.when((place == role) & (i == step))(body)

    def pick(i, which):
        found = jnp.int32(0)
        for role, rounds in enumerate(ROUNDS):
            for step, entry in enumerate(rounds):
                if entry[which]:
                    found = found + jnp.where((place == role) & (i == step), entry[which], 0)
        return found

    def project(e, base):
        column = columns[cut(base, count), e : e + 1]

        def tile(t, carry):
            at = pl.ds(pl.multiple_of(t * LANES, LANES), LANES)
            block = rows[cut(base, count)]
            g = jnp.dot(block, gate[e, :, at], preferred_element_type=jnp.float32)
            v = jnp.dot(block, up[e, :, at], preferred_element_type=jnp.float32)
            h = g / (1.0 + jnp.exp(-g)) * v * column
            hidden[:, pl.ds(pl.multiple_of(e * ff + t * LANES, LANES), LANES)] = h.astype(jnp.bfloat16)
            return carry

        lax.fori_loop(0, ff // LANES, tile, 0, unroll=True)

    def spread(low, high, base):
        def tile(t, carry):
            at = pl.ds(pl.multiple_of(t * LANES, LANES), LANES)
            result = jnp.dot(hidden[...], down[:, at], preferred_element_type=jnp.float32)
            part[cut(base, count), at] = result.astype(jnp.bfloat16)
            return carry

        lax.fori_loop(low, high, tile, 0, unroll=True)

    def step(i, carry):
        o, h = pick(i, 0), pick(i, 1)
        base = owner_of(o) * SIDE * count + h * count
        tiles = width // LANES
        for p in range(PIECES):
            talk(p, i)

            @pl.when(i == 0)
            def _():
                for load in loads[2 * p : 2 * p + 2] if p < local else loads[2 * local :] if p == local else []:
                    load.wait()

            if p < local:
                project(p, base)
            else:
                share = tiles // (PIECES - local)
                spread((p - local) * share, (p - local + 1) * share, base)
        return carry

    lax.fori_loop(0, steps, step, 0)

    def ending(role):
        for piece in acts[role][steps * PIECES :]:
            for action in piece:
                act(role, *action)
        for way in (AWAY, HOME, ACROSS):
            for kind, sems in ((1, token_send), (2, result_send)):
                sent = sum(a[4] for piece in acts[role] for a in piece if a[0] == kind and a[5] == way)
                if sent:
                    all_of = rows.at[pl.ds(0, sent * size)]
                    remote(all_of, all_of, sems.at[way], token_recv.at[0], device(way)).wait_send()

        passed = sum(beyond(role, way) for o in range(depth) for way in onward(role, o))
        given = shares.at[pl.ds(0, passed)]
        remote(given, given, share_send.at[0], share_recv.at[0], device(ACROSS)).wait_send()

    for role in range(len(acts)):
        pl.when(place == role)(functools.partial(ending, role))
    remote(factors, factors, factor_send.at[0], factor_recv.at[0], device(ACROSS)).wait_send()


def fused(tokens, expert_ids, gate_nums, w_gate, w_up, w_down, n):
    count, width = tokens.shape
    local, _, ff = w_gate.shape
    depth = n // SIDE
    everyone = n * count
    choices = (expert_ids * int(denominator) + gate_nums).T
    kind = tokens.dtype
    dma = pltpu.SemaphoreType.DMA
    vmem = pl.BlockSpec(memory_space=pltpu.VMEM)
    hbm = pl.BlockSpec(memory_space=pl.ANY)
    return pl.pallas_call(
        functools.partial(kernel, n, local),
        out_shape=jax.ShapeDtypeStruct((count, width), kind),
        in_specs=[vmem, hbm, hbm, hbm, hbm],
        out_specs=vmem,
        scratch_shapes=[
            pltpu.VMEM((everyone, width), kind),
            pltpu.VMEM((depth * n, local, count), jnp.float32),
            pltpu.VMEM((depth, local, count), jnp.float32),
            pltpu.VMEM((everyone, local + -local % 8), jnp.float32),
            pltpu.VMEM((local, width, ff), kind),
            pltpu.VMEM((local, width, ff), kind),
            pltpu.VMEM((local * ff, width), kind),
            pltpu.VMEM((count, local * ff), kind),
            pltpu.VMEM((everyone, width), kind),
            pltpu.VMEM((2 * everyone, width), kind),
            pltpu.VMEM((depth * count, width), kind),
            dma((2 + 3 * local,)),
            dma((1,)), dma((depth,)), dma((1,)), dma((depth,)),
            dma((3,)), dma((n * UNITS,)),
            dma((3,)), dma((2 * n * UNITS,)), dma((depth * UNITS,)),
        ],
        compiler_params=pltpu.CompilerParams(
            collective_id=0, has_side_effects=True, vmem_limit_bytes=VMEM
        ),
    )(choices, tokens, w_gate, w_up, w_down)


def plain(tokens, expert_ids, gate_nums, w_gate, w_up, w_down, n):
    weight = expert_weights(expert_ids, gate_nums, w_gate.shape[0] * n)
    weights = lax.all_to_all(weight, "ep", split_axis=1, concat_axis=0, tiled=True)
    rows = lax.all_gather(tokens, "ep", axis=0, tiled=True)
    gate = jnp.einsum("td,xdf->xtf", rows, w_gate, preferred_element_type=jnp.float32)
    up = jnp.einsum("td,xdf->xtf", rows, w_up, preferred_element_type=jnp.float32)
    hidden = (jax.nn.silu(gate) * up * weights.T[:, :, None]).astype(jnp.bfloat16)
    result = jnp.einsum("xtf,xfd->td", hidden, w_down, preferred_element_type=jnp.float32)
    return lax.psum_scatter(
        result.astype(jnp.bfloat16), "ep", scatter_dimension=0, tiled=True
    )


def shards(n, tokens, expert_ids, gate_nums, w_gate, w_up, w_down):
    count, width = tokens.shape
    local, _, ff = w_gate.shape
    held = 5 * n * count * width + 3 * local * width * ff + 2 * count * local * ff
    fits = 2 * held < VMEM - 4 * 2**20
    planned = n == 2 * SIDE * len(SENDS) and PIECES == local + 2
    shaped = count % (16 * UNITS) == 0 and count % 128 == 0 and ff % LANES == 0 and width % (2 * LANES) == 0
    plan = fused if fits and planned and shaped else plain
    return plan(tokens, expert_ids, gate_nums, w_gate, w_up, w_down, n)


def solution(mesh):
    placed = (
        P(("dp", "ep"), None),
        P(("dp", "ep"), None),
        P(("dp", "ep"), None),
        P("ep", None, None),
        P("ep", None, None),
        P("ep", None, None),
    )
    return jax.shard_map(
        functools.partial(shards, mesh.shape["ep"]),
        mesh=mesh, in_specs=placed, out_specs=P(("dp", "ep"), None), check_vma=False,
    )
```

```python
import functools

import jax
import jax.numpy as jnp
from jax import lax
from jax.experimental import pallas as pl
from jax.experimental.pallas import tpu as pltpu
from jax.sharding import PartitionSpec as P

denominator = 1024.0
SIDE = 2
LANES = 256
VMEM = 53 * 2**20

AWAY, HOME, ACROSS = 0, 1, 2
UNITS = 8
PIECES = 4
ROUNDS = (
    ((1, 0), (2, 0), (0, 0), (0, 1), (3, 0), (3, 1), (2, 1), (1, 1)),
    ((0, 0), (1, 0), (3, 0), (2, 0), (3, 1), (2, 1), (0, 1), (1, 1)),
)
SENDS = (
    (
        (500010, 100020, 100012, 100312, 100220, 100422, 101010, 100420, 510010, 110022, 110222, 101420,
         520010, 100620, 120022, 111010, 530010, 120222),
        (),
        (),
        (),
        (211212, 211020, 211310, 100622, 130012, 210020),
        (),
        (),
        (),
        (),
        (221012, 221110, 221222, 220110),
        (),
        (130212,),
        (),
        (),
        (220010,),
        (),
        (130422, 201710, 220220, 210220, 130622),
        (),
        (),
        (),
        (231012, 231110, 231212, 231310, 120422),
        (),
        (230020,),
        (),
        (231422, 231610, 231712, 230220, 201012),
        (),
        (),
        (),
        (230420, 221422, 221622, 230620, 201212),
        (220420,),
        (201112,),
        (),
        (211610, 211422, 220620, 211712, 210610, 201312, 201422, 300010, 300110, 210420, 201612, 300210,
         210710, 300310, 300410, 300510, 300710, 300610),
    ),
    (
        (510010, 110020, 110021, 110112, 110222, 110220, 110221, 110422, 500010, 520010, 100020, 120021,
         100112, 100220, 120221, 100222, 111210, 530010, 130022, 130021, 101111, 110622, 100420),
        (101220, 101211, 120022),
        (),
        (130221,),
        (131111, 100620, 130422, 110420),
        (100622, 130421),
        (131311,),
        (110620,),
        (),
        (120312,),
        (130621,),
        (),
        (231010, 120422, 120421, 101620, 231210, 120622, 120621),
        (),
        (201012,),
        (110421,),
        (220020, 221212),
        (221020,),
        (121621, 201212),
        (220310, 211212),
        (),
        (231712, 110621),
        (220210,),
        (221310,),
        (231112,),
        (111421, 221610),
        (231312,),
        (231420, 221422),
        (),
        (201712, 111621),
        (310210,),
        (230020,),
        (231612, 201111, 221712, 201311, 230220, 201611, 201422, 211022, 230420, 200021, 211312, 230620,
         211422, 200221, 220420, 200421, 211622, 310010, 310110, 310310, 200621, 220620, 310410, 310510,
         310610, 310710),
    ),
)


def expert_weights(expert_ids, gate_nums, experts):
    gates = gate_nums.astype(jnp.float32) / denominator
    labels = jnp.arange(experts, dtype=jnp.int32)
    onehot = expert_ids[:, :, None] == labels[None, None, :]
    return jnp.sum(jnp.where(onehot, gates[:, :, None], 0.0), axis=1)


def digits(code):
    return tuple(code // 10**k % 10 for k in range(5, -1, -1))


def script(depth):
    tokens, results = [{} for _ in SENDS], [{} for _ in SENDS]
    for role, pieces in enumerate(SENDS):
        for kind, o, r, u, units, way in [digits(code) for piece in pieces for code in piece]:
            there, o, r, way = role + (way == AWAY) - (way == HOME), o, r ^ (way == ACROSS), way
            if there == depth // 2:
                there, o, way = role, depth - 1 - o, HOME
            for v in range(u, u + units):
                if kind == 1:
                    tokens[there][o, r, v] = (u, units)
                if kind == 2:
                    results[there].setdefault((o, r, v), []).append((way, u, units))
    acts = []
    for role, pieces in enumerate(SENDS):
        seen, heard, mine = set(), set(), []
        for index, piece in enumerate(pieces):
            found = []

            def need(o, r, u):
                if (o, r) != (role, 0) and (o, r, u) not in seen:
                    first, units = tokens[role][o, r, u]
                    seen.update((o, r, first + v) for v in range(units))
                    found.append((0, o, r, first, units, ACROSS, ()))

            for kind, o, r, u, units, way in [digits(code) for code in piece]:
                ways = []
                for v in range(u, u + units):
                    if kind == 1:
                        need(o, r, v)
                    if kind not in (2, 3):
                        continue
                    for source, first, size in results[role].get((o, r, v), []):
                        if (source, o, r, first) not in heard:
                            heard.add((source, o, r, first))
                            found.append((4, o, r, first, size, source, ()))
                    ways.append(tuple(source for source, _, _ in results[role].get((o, r, v), [])))
                found.append((kind, o, r, u, units, way, tuple(ways)))
            if index % PIECES == 0 and index < len(ROUNDS[role]) * PIECES:
                o, h = ROUNDS[role][index // PIECES]
                if o not in [entry[0] for entry in ROUNDS[role][: index // PIECES]]:
                    found.append((6, o, 0, 0, 0, 0, ()))
                for r in range(SIDE):
                    for u in range(h * UNITS // 2, (h + 1) * UNITS // 2):
                        need(o, r, u)
            mine.append(found)
        acts.append(mine)
    return acts


def kernel(
    n, local,
    choices, tokens, w_gate, w_up, w_down, out,
    rows, shares, factors, columns, gate, up, down, hidden, part, line, side,
    load_sem, share_send, share_recv, factor_send, factor_recv, token_send, token_recv, result_send, line_recv, side_recv,
):
    depth = n // SIDE
    me = lax.axis_index("ep")
    z, y = me // SIDE, me % SIDE
    flip = z // (depth // 2)
    place = z + flip * (depth - 1 - 2 * z)
    count, width = tokens.shape
    ff = w_gate.shape[2]
    size = count // UNITS
    half = count // 2
    spots = depth * SIDE * UNITS
    acts = script(depth)
    steps = len(ROUNDS[0])

    def owner_of(o):
        return o + flip * (depth - 1 - 2 * o)

    def row_of(r):
        return y if r == 0 else 1 - y

    def offset(o, r, u):
        return owner_of(o) * SIDE * count + u * size // half * count + row_of(r) * half + u * size % half

    def spot(o, r, u):
        return (owner_of(o) * SIDE + row_of(r)) * UNITS + u

    def cut(start, extent=size):
        return pl.ds(pl.multiple_of(start, size), extent)

    def heading(way):
        return flip if way == AWAY else 1 - flip

    def device(way):
        return z * SIDE + 1 - y if way == ACROSS else me + SIDE * (1 - 2 * heading(way))

    def remote(source, target, send, recv, there):
        return pltpu.make_async_remote_copy(
            src_ref=source, dst_ref=target, send_sem=send, recv_sem=recv,
            device_id={"ep": there}, device_id_type=pl.DeviceIdType.MESH,
        )

    def token_copy(o, r, u, units, way):
        ref = rows.at[cut(offset(o, r, u), units * size)]
        return remote(ref, ref, token_send.at[way], token_recv.at[spot(o, r, u)], device(way))

    def landing(o, r, u, units, way):
        if way == ACROSS:
            start, recv = owner_of(o) * count + u * size, side_recv.at[owner_of(o) * UNITS + u]
            return side.at[cut(start, units * size)], recv
        start = heading(way) * (depth * SIDE * count) + offset(o, r, u)
        return line.at[cut(start, units * size)], line_recv.at[heading(way) * spots + spot(o, r, u)]

    def result_copy(o, r, u, units, way):
        target, recv = landing(o, r, u, units, way)
        source = part.at[cut(offset(o, r, u), units * size)]
        return remote(source, target, result_send.at[way], recv, device(way))

    barrier = pltpu.get_barrier_semaphore()
    def greet(there):
        pl.semaphore_signal(barrier, inc=1, device_id={"ep": there}, device_id_type=pl.DeviceIdType.MESH)

    greet(device(ACROSS))
    greet(device(AWAY))
    pl.when(place > 0)(lambda: greet(device(HOME)))

    own = []
    for h in range(2):
        start = z * SIDE * count + h * count + y * half
        own.append(
            pltpu.make_async_copy(tokens.at[pl.ds(h * half, half)], rows.at[cut(start, half)], load_sem.at[h])
        )
    loads = []
    for e in range(local):
        loads.append(pltpu.make_async_copy(w_gate.at[e], gate.at[e], load_sem.at[2 + 3 * e]))
        loads.append(pltpu.make_async_copy(w_up.at[e], up.at[e], load_sem.at[3 + 3 * e]))
    for e in range(local):
        loads.append(pltpu.make_async_copy(w_down.at[e], down.at[pl.ds(e * ff, ff)], load_sem.at[4 + 3 * e]))
    for load in own + loads:
        load.start()

    ids = choices[...] // int(denominator)
    gates = (choices[...] % int(denominator)).astype(jnp.float32) / denominator
    for d in range(n):
        for e in range(local):
            chosen = jnp.where(ids == d * local + e, gates, 0.0)
            shares[z * n + d, e : e + 1] = jnp.sum(chosen, axis=0, keepdims=True)

    pl.when(place == 0)(lambda: pl.semaphore_wait(barrier, 2))
    pl.when(place > 0)(lambda: pl.semaphore_wait(barrier, 3))
    for load in own:
        load.wait()

    def added(o, r, u, units, ways):
        total = part[cut(offset(o, r, u), units * size)].astype(jnp.float32)
        for way in ways:
            total = total + landing(o, r, u, units, way)[0][...].astype(jnp.float32)
        return total

    def onward(role, o):
        return [AWAY] * (o <= role) + [HOME] * (o >= role and role > 0)

    def beyond(role, way):
        return SIDE * (depth - 1 - role if way == AWAY else role)

    def share_copy(role, o, way):
        first = SIDE * (z + 1) if way == AWAY else 0
        mirrored = 0 if way == AWAY else SIDE * (z + 1)
        ref = shares.at[pl.ds(owner_of(o) * n + jnp.where(flip == 0, first, mirrored), beyond(role, way))]
        return remote(ref, ref, share_send.at[0], share_recv.at[owner_of(o)], device(way))

    def factor_copy(o):
        there = device(ACROSS)
        return remote(
            shares.at[owner_of(o) * n + there], factors.at[owner_of(o)], factor_send.at[0], factor_recv.at[owner_of(o)], there
        )

    def pass_on(role, o):
        if o != role:
            extent = SIDE * (depth - role if o < role else role + 1)
            start = jnp.where((flip == 0) == (o < role), SIDE * z, 0)
            ref = shares.at[pl.ds(owner_of(o) * n + start, extent)]
            remote(ref, ref, share_send.at[0], share_recv.at[owner_of(o)], device(ACROSS)).wait_recv()
        for way in onward(role, o):
            share_copy(role, o, way).start()
        factor_copy(o).start()

    def lay_out(o):
        factor_copy(o).wait_recv()
        for r, block in ((0, shares[owner_of(o) * n + me]), (1, factors[owner_of(o)])):
            turned = jnp.concatenate([block, jnp.zeros((-local % 8, count), jnp.float32)], axis=0).T
            for h in range(2):
                start = owner_of(o) * SIDE * count + h * count + row_of(r) * half
                columns[cut(start, half)] = turned[h * half : (h + 1) * half]

    def act(role, kind, o, r, u, units, way, ways):
        if kind == 0:
            token_copy(o, r, u, units, way).wait_recv()
        elif kind == 1:
            token_copy(o, r, u, units, way).start()
        elif kind == 4:
            target, recv = landing(o, r, u, units, way)
            remote(target, target, result_send.at[way], recv, device(way)).wait_recv()
        elif kind == 5:
            pass_on(role, o)
        elif kind == 6:
            lay_out(o)
        elif kind == 3:
            out[pl.ds(u * size, size)] = added(o, r, u, units, ways[0]).astype(out.dtype)
        else:
            together = units if len(set(ways)) == 1 else 1
            for v in range(0, units, together):
                if ways[v]:
                    total = added(o, r, u + v, together, ways[v])
                    part[cut(offset(o, r, u + v), together * size)] = total.astype(part.dtype)
            result_copy(o, r, u, units, way).start()

    def branch(index, low, high, todo):
        if not any(k in todo for k in range(low, high)):
            return
        if high - low == 1:
            todo[low]()
            return
        mid = (low + high) // 2
        lax.cond(
            index < mid, lambda: branch(index, low, mid, todo), lambda: branch(index, mid, high, todo)
        )

    def talk(p, i):
        def speak(role, piece):
            for action in piece:
                act(role, *action)

        def in_role(role):
            found = {k: acts[role][k * PIECES + p] for k in range(steps)}
            branch(i, 0, steps, {k: functools.partial(speak, role, piece) for k, piece in found.items() if piece})

        branch(place, 0, len(acts), {role: functools.partial(in_role, role) for role in range(len(acts))})

    def pick(i):
        def halve(index, low, high, value):
            if high - low == 1:
                return value(low)
            mid = (low + high) // 2
            return jnp.where(index < mid, halve(index, low, mid, value), halve(index, mid, high, value))

        def in_role(role):
            return halve(i, 0, steps, lambda k: jnp.int32(ROUNDS[role][k][0] * 2 + ROUNDS[role][k][1]))

        return halve(place, 0, len(ROUNDS), in_role)

    def project(e, base):
        column = columns[cut(base, count), e : e + 1]

        def tile(t, carry):
            at = pl.ds(pl.multiple_of(t * LANES, LANES), LANES)
            block = rows[cut(base, count)]
            g = jnp.dot(block, gate[e, :, at], preferred_element_type=jnp.float32)
            v = jnp.dot(block, up[e, :, at], preferred_element_type=jnp.float32)
            h = g / (1.0 + jnp.exp(-g)) * v * column
            hidden[:, pl.ds(pl.multiple_of(e * ff + t * LANES, LANES), LANES)] = h.astype(jnp.bfloat16)
            return carry

        lax.fori_loop(0, ff // LANES, tile, 0, unroll=True)

    def spread(low, high, base):
        def tile(t, carry):
            at = pl.ds(pl.multiple_of(t * LANES, LANES), LANES)
            result = jnp.dot(hidden[...], down[:, at], preferred_element_type=jnp.float32)
            part[cut(base, count), at] = result.astype(jnp.bfloat16)
            return carry

        lax.fori_loop(low, high, tile, 0, unroll=True)

    def step(i, carry):
        code = pick(i)
        o, h = code // 2, code % 2
        base = owner_of(o) * SIDE * count + h * count
        tiles = width // LANES
        for p in range(PIECES):
            talk(p, i)

            @pl.when(i == 0)
            def _():
                for load in loads[2 * p : 2 * p + 2] if p < local else loads[2 * local :] if p == local else []:
                    load.wait()

            if p < local:
                project(p, base)
            else:
                share = tiles // (PIECES - local)
                spread((p - local) * share, (p - local + 1) * share, base)
        return carry

    lax.fori_loop(0, steps, step, 0)

    def ending(role):
        for piece in acts[role][steps * PIECES :]:
            for action in piece:
                act(role, *action)
        for way in (AWAY, HOME, ACROSS):
            for kind, sems in ((1, token_send), (2, result_send)):
                sent = sum(a[4] for piece in acts[role] for a in piece if a[0] == kind and a[5] == way)
                if sent:
                    all_of = rows.at[pl.ds(0, sent * size)]
                    remote(all_of, all_of, sems.at[way], token_recv.at[0], device(way)).wait_send()

        passed = sum(beyond(role, way) for o in range(depth) for way in onward(role, o))
        given = shares.at[pl.ds(0, passed)]
        remote(given, given, share_send.at[0], share_recv.at[0], device(ACROSS)).wait_send()

    for role in range(len(acts)):
        pl.when(place == role)(functools.partial(ending, role))
    remote(factors, factors, factor_send.at[0], factor_recv.at[0], device(ACROSS)).wait_send()


def fused(tokens, expert_ids, gate_nums, w_gate, w_up, w_down, n):
    count, width = tokens.shape
    local, _, ff = w_gate.shape
    depth = n // SIDE
    everyone = n * count
    choices = (expert_ids * int(denominator) + gate_nums).T
    kind = tokens.dtype
    dma = pltpu.SemaphoreType.DMA
    vmem = pl.BlockSpec(memory_space=pltpu.VMEM)
    hbm = pl.BlockSpec(memory_space=pl.ANY)
    return pl.pallas_call(
        functools.partial(kernel, n, local),
        out_shape=jax.ShapeDtypeStruct((count, width), kind),
        in_specs=[vmem, hbm, hbm, hbm, hbm],
        out_specs=vmem,
        scratch_shapes=[
            pltpu.VMEM((everyone, width), kind),
            pltpu.VMEM((depth * n, local, count), jnp.float32),
            pltpu.VMEM((depth, local, count), jnp.float32),
            pltpu.VMEM((everyone, local + -local % 8), jnp.float32),
            pltpu.VMEM((local, width, ff), kind),
            pltpu.VMEM((local, width, ff), kind),
            pltpu.VMEM((local * ff, width), kind),
            pltpu.VMEM((count, local * ff), kind),
            pltpu.VMEM((everyone, width), kind),
            pltpu.VMEM((2 * everyone, width), kind),
            pltpu.VMEM((depth * count, width), kind),
            dma((2 + 3 * local,)),
            dma((1,)), dma((depth,)), dma((1,)), dma((depth,)),
            dma((3,)), dma((n * UNITS,)),
            dma((3,)), dma((2 * n * UNITS,)), dma((depth * UNITS,)),
        ],
        compiler_params=pltpu.CompilerParams(
            collective_id=0, has_side_effects=True, vmem_limit_bytes=VMEM
        ),
    )(choices, tokens, w_gate, w_up, w_down)


def plain(tokens, expert_ids, gate_nums, w_gate, w_up, w_down, n):
    weight = expert_weights(expert_ids, gate_nums, w_gate.shape[0] * n)
    weights = lax.all_to_all(weight, "ep", split_axis=1, concat_axis=0, tiled=True)
    rows = lax.all_gather(tokens, "ep", axis=0, tiled=True)
    gate = jnp.einsum("td,xdf->xtf", rows, w_gate, preferred_element_type=jnp.float32)
    up = jnp.einsum("td,xdf->xtf", rows, w_up, preferred_element_type=jnp.float32)
    hidden = (jax.nn.silu(gate) * up * weights.T[:, :, None]).astype(jnp.bfloat16)
    result = jnp.einsum("xtf,xfd->td", hidden, w_down, preferred_element_type=jnp.float32)
    return lax.psum_scatter(
        result.astype(jnp.bfloat16), "ep", scatter_dimension=0, tiled=True
    )


def shards(n, tokens, expert_ids, gate_nums, w_gate, w_up, w_down):
    count, width = tokens.shape
    local, _, ff = w_gate.shape
    held = 5 * n * count * width + 3 * local * width * ff + 2 * count * local * ff
    fits = 2 * held < VMEM - 4 * 2**20
    planned = n == 2 * SIDE * len(SENDS) and PIECES == local + 2
    shaped = count % (16 * UNITS) == 0 and count % 128 == 0 and ff % LANES == 0 and width % (2 * LANES) == 0
    plan = fused if fits and planned and shaped else plain
    return plan(tokens, expert_ids, gate_nums, w_gate, w_up, w_down, n)


def solution(mesh):
    placed = (
        P(("dp", "ep"), None),
        P(("dp", "ep"), None),
        P(("dp", "ep"), None),
        P("ep", None, None),
        P("ep", None, None),
        P("ep", None, None),
    )
    return jax.shard_map(
        functools.partial(shards, mesh.shape["ep"]),
        mesh=mesh, in_specs=placed, out_specs=P(("dp", "ep"), None), check_vma=False,
    )
```
